16 devices in a mesh: tp: 2 (over z), fsdp: 8 (over y, x, core).
Axes of the slice: x: 2, y: 2, z: 2, core: 2. Of those that a mesh axis runs over, the one named last changes fastest.
Arguments:
- x_in: bfloat16 [96, 512, 768], P('fsdp', 'tp')
- dy_in: bfloat16 [96, 512, 768], P('fsdp', 'tp')
- ln1_gain: bfloat16 [768], P('fsdp')
- ln1_bias: bfloat16 [768], P('fsdp')
- w_qkv: bfloat16 [768, 12, 192], P('fsdp', 'tp')
- b_qkv: bfloat16 [2304], P(('tp', 'fsdp'))
- w_out: bfloat16 [768, 768], P(('tp', 'fsdp'))
- b_out: bfloat16 [768], P('fsdp')
- ln2_gain: bfloat16 [768], P('fsdp')
- ln2_bias: bfloat16 [768], P('fsdp')
- w_up: bfloat16 [768, 3072], P('fsdp', 'tp')
- b_up: bfloat16 [3072], P(('tp', 'fsdp'))
- w_down: bfloat16 [3072, 768], P(('tp', 'fsdp'))
- b_down: bfloat16 [768], P('fsdp')
Outputs:
- output 1: bfloat16 [96, 512, 768], P('fsdp', 'tp')
- output 2: bfloat16 [96, 512, 768], P('fsdp', 'tp')
- output 3: float32 [768], P('fsdp')
- output 4: float32 [768], P('fsdp')
- output 5: float32 [768, 12, 192], P('fsdp', 'tp')
- output 6: float32 [2304], P(('tp', 'fsdp'))
- output 7: float32 [768, 768], P(('tp', 'fsdp'))
- output 8: float32 [768], P('fsdp')
- output 9: float32 [768], P('fsdp')
- output 10: float32 [768], P('fsdp')
- output 11: float32 [768, 3072], P('fsdp', 'tp')
- output 12: float32 [3072], P(('tp', 'fsdp'))
- output 13: float32 [3072, 768], P(('tp', 'fsdp'))
- output 14: float32 [768], P('fsdp')
All inputs are finite; a program needn't handle non-finite values.
Results may differ from the reference program's by a relative error of at most 0.00805824.
Values are sent between devices in bfloat16 or wider.
A program may use at most 1 GiB of HBM per device.

```python
import jax
import jax.numpy as jnp
from jax import lax

BATCH = 96
SEQ = 512
D_MODEL = 768
HEADS = 12
HEAD_DIM = D_MODEL // HEADS
FFN = 4 * D_MODEL


def setup_inputs(seed: int = 0) -> dict:
    keys = jax.random.split(jax.random.key(seed), 14)

    def normal(key, shape, scale):
        return scale * jax.random.normal(key, shape, jnp.float32)

    act_shape = (BATCH, SEQ, D_MODEL)
    return {
        'x_in': normal(keys[0], act_shape, 1.0).astype(jnp.bfloat16),
        'dy_in': normal(keys[1], act_shape, 1.0).astype(jnp.bfloat16),
        'ln1_gain': (1.0 + normal(keys[2], (D_MODEL,), 0.2)).astype(jnp.bfloat16),
        'ln1_bias': normal(keys[3], (D_MODEL,), 0.2).astype(jnp.bfloat16),
        'w_qkv': normal(keys[4], (D_MODEL, HEADS, 3 * HEAD_DIM), D_MODEL ** -0.5).astype(jnp.bfloat16),
        'b_qkv': normal(keys[5], (3 * D_MODEL,), 0.3).astype(jnp.bfloat16),
        'w_out': normal(keys[6], (D_MODEL, D_MODEL), D_MODEL ** -0.5).astype(jnp.bfloat16),
        'b_out': normal(keys[7], (D_MODEL,), 0.2).astype(jnp.bfloat16),
        'ln2_gain': (1.0 + normal(keys[8], (D_MODEL,), 0.2)).astype(jnp.bfloat16),
        'ln2_bias': normal(keys[9], (D_MODEL,), 0.2).astype(jnp.bfloat16),
        'w_up': normal(keys[10], (D_MODEL, FFN), D_MODEL ** -0.5).astype(jnp.bfloat16),
        'b_up': normal(keys[11], (FFN,), 0.3).astype(jnp.bfloat16),
        'w_down': normal(keys[12], (FFN, D_MODEL), FFN ** -0.5).astype(jnp.bfloat16),
        'b_down': normal(keys[13], (D_MODEL,), 0.2).astype(jnp.bfloat16),
    }


def layer_norm(values, gain, bias):
    average = jnp.mean(values, axis=-1, keepdims=True)
    centred = values - average
    variance = jnp.mean(centred * centred, axis=-1, keepdims=True)
    return centred * lax.rsqrt(variance + 1e-5) * gain + bias


def gelu_tanh(values):
    return jax.nn.gelu(values, approximate=True)


def head_probs(q_head, k_head):
    scores = jnp.dot(q_head, k_head.T, preferred_element_type=jnp.float32) * HEAD_DIM ** -0.5
    causal = jnp.arange(SEQ)[:, None] >= jnp.arange(SEQ)[None, :]
    return jax.nn.softmax(jnp.where(causal, scores, -1e30), axis=-1)


def head_forward(qkv_head):
    q_head = qkv_head[:, :HEAD_DIM]
    k_head = qkv_head[:, HEAD_DIM:2 * HEAD_DIM]
    v_head = qkv_head[:, 2 * HEAD_DIM:]
    attn_prob = head_probs(q_head, k_head)
    return jnp.dot(attn_prob.astype(jnp.bfloat16), v_head, preferred_element_type=jnp.float32).astype(jnp.bfloat16)


def head_backward(pair):
    qkv_head, d_att = pair
    q_head = qkv_head[:, :HEAD_DIM]
    k_head = qkv_head[:, HEAD_DIM:2 * HEAD_DIM]
    v_head = qkv_head[:, 2 * HEAD_DIM:]
    attn_prob = head_probs(q_head, k_head)
    prob_low = attn_prob.astype(jnp.bfloat16)
    d_prob = jnp.dot(d_att, v_head.T, preferred_element_type=jnp.float32)
    d_v = jnp.dot(prob_low.T, d_att, preferred_element_type=jnp.float32)
    d_scores = attn_prob * (d_prob - jnp.sum(d_prob * attn_prob, axis=-1, keepdims=True))
    d_scores_low = (d_scores * HEAD_DIM ** -0.5).astype(jnp.bfloat16)
    d_q = jnp.dot(d_scores_low, k_head, preferred_element_type=jnp.float32)
    d_k = jnp.dot(d_scores_low.T, q_head, preferred_element_type=jnp.float32)
    return jnp.concatenate([d_q, d_k, d_v], axis=-1)


def sequence_pass(x_seq, dy_seq, weights):
    ln1_gain, ln1_bias, w_qkv, b_qkv, w_out, b_out, ln2_gain, ln2_bias, w_up, b_up, w_down, b_down = weights
    qkv_matrix = w_qkv.reshape(D_MODEL, 3 * D_MODEL)
    x_wide = x_seq.astype(jnp.float32)
    ln1_val, ln1_back = jax.vjp(layer_norm, x_wide, ln1_gain.astype(jnp.float32), ln1_bias.astype(jnp.float32))
    h_one = ln1_val.astype(jnp.bfloat16)
    qkv_flat = (jnp.dot(h_one, qkv_matrix, preferred_element_type=jnp.float32) + b_qkv.astype(jnp.float32)).astype(jnp.bfloat16)
    qkv_heads = qkv_flat.reshape(SEQ, HEADS, 3 * HEAD_DIM).transpose(1, 0, 2)
    att_heads = lax.map(head_forward, qkv_heads)
    att_out = att_heads.transpose(1, 0, 2).reshape(SEQ, D_MODEL)
    residual = x_wide + jnp.dot(att_out, w_out, preferred_element_type=jnp.float32) + b_out.astype(jnp.float32)
    ln2_val, ln2_back = jax.vjp(layer_norm, residual, ln2_gain.astype(jnp.float32), ln2_bias.astype(jnp.float32))
    h_two = ln2_val.astype(jnp.bfloat16)
    up_pre = jnp.dot(h_two, w_up, preferred_element_type=jnp.float32) + b_up.astype(jnp.float32)
    gelu_out, gelu_back = jax.vjp(gelu_tanh, up_pre)
    gelu_low = gelu_out.astype(jnp.bfloat16)
    y_seq = (residual + jnp.dot(gelu_low, w_down, preferred_element_type=jnp.float32) + b_down.astype(jnp.float32)).astype(jnp.bfloat16)
    dy_wide = dy_seq.astype(jnp.float32)
    g_b_down = jnp.sum(dy_wide, axis=0)
    g_w_down = jnp.dot(gelu_low.T, dy_seq, preferred_element_type=jnp.float32)
    d_up = gelu_back(jnp.dot(dy_seq, w_down.T, preferred_element_type=jnp.float32))[0]
    d_up_low = d_up.astype(jnp.bfloat16)
    g_b_up = jnp.sum(d_up, axis=0)
    g_w_up = jnp.dot(h_two.T, d_up_low, preferred_element_type=jnp.float32)
    d_res_ln, g_ln2_gain, g_ln2_bias = ln2_back(jnp.dot(d_up_low, w_up.T, preferred_element_type=jnp.float32))
    d_resid = dy_wide + d_res_ln
    g_b_out = jnp.sum(d_resid, axis=0)
    d_resid_low = d_resid.astype(jnp.bfloat16)
    g_w_out = jnp.dot(att_out.T, d_resid_low, preferred_element_type=jnp.float32)
    d_att = jnp.dot(d_resid_low, w_out.T, preferred_element_type=jnp.float32).astype(jnp.bfloat16)
    d_att_heads = d_att.reshape(SEQ, HEADS, HEAD_DIM).transpose(1, 0, 2)
    d_qkv_heads = lax.map(head_backward, (qkv_heads, d_att_heads))
    d_qkv = d_qkv_heads.transpose(1, 0, 2).reshape(SEQ, 3 * D_MODEL)
    g_b_qkv = jnp.sum(d_qkv, axis=0)
    d_qkv_low = d_qkv.astype(jnp.bfloat16)
    g_w_qkv = jnp.dot(h_one.T, d_qkv_low, preferred_element_type=jnp.float32).reshape(D_MODEL, HEADS, 3 * HEAD_DIM)
    d_x_ln, g_ln1_gain, g_ln1_bias = ln1_back(jnp.dot(d_qkv_low, qkv_matrix.T, preferred_element_type=jnp.float32))
    dx_seq = (d_resid + d_x_ln).astype(jnp.bfloat16)
    seq_grads = (g_ln1_gain, g_ln1_bias, g_w_qkv, g_b_qkv, g_w_out, g_b_out, g_ln2_gain, g_ln2_bias, g_w_up, g_b_up, g_w_down, g_b_down)
    return y_seq, dx_seq, seq_grads


def reference(x_in, dy_in, ln1_gain, ln1_bias, w_qkv, b_qkv, w_out, b_out, ln2_gain, ln2_bias, w_up, b_up, w_down, b_down):
    weights = (ln1_gain, ln1_bias, w_qkv, b_qkv, w_out, b_out, ln2_gain, ln2_bias, w_up, b_up, w_down, b_down)
    zero_grads = tuple(jnp.zeros(tensor.shape, jnp.float32) for tensor in weights)

    def body(carry, pair):
        y_seq, dx_seq, seq_grads = sequence_pass(pair[0], pair[1], weights)
        return tuple(total + step for total, step in zip(carry, seq_grads)), (y_seq, dx_seq)

    grad_sums, act_outs = lax.scan(body, zero_grads, (x_in, dy_in))
    return (act_outs[0], act_outs[1], grad_sums[0], grad_sums[1], grad_sums[2], grad_sums[3], grad_sums[4], grad_sums[5], grad_sums[6], grad_sums[7], grad_sums[8], grad_sums[9], grad_sums[10], grad_sums[11])
```

```python
import functools
import math

import jax
import jax.numpy as jnp
from jax import lax
from jax.experimental import pallas as pl
from jax.experimental.pallas import tpu as pltpu
from jax.sharding import Mesh, PartitionSpec as P

F32 = jnp.float32
BF16 = jnp.bfloat16
FSDP = ('y', 'x', 'core')
ALL = ('tp',) + FSDP
SWAP = [(0, 1), (1, 0)]


def layer_norm(values, gain, bias):
    average = jnp.mean(values, axis=-1, keepdims=True)
    centred = values - average
    variance = jnp.mean(centred * centred, axis=-1, keepdims=True)
    return centred * lax.rsqrt(variance + 1e-5) * gain + bias


def gelu_tanh(values):
    return jax.nn.gelu(values, approximate=True)


def dot_nn(a, b):
    return lax.dot_general(a, b, (((1,), (0,)), ((), ())), preferred_element_type=F32)


def dot_nt(a, b):
    return lax.dot_general(a, b, (((1,), (1,)), ((), ())), preferred_element_type=F32)


def dot_tn(a, b):
    return lax.dot_general(a, b, (((0,), (0,)), ((), ())), preferred_element_type=F32)


def attend_kernel(head_dim, side_ref, qkv_ref, out_ref):
    side = side_ref[0]
    half = qkv_ref.shape[2]
    exponent = head_dim ** -0.5 * math.log2(math.e)
    diag = lax.broadcasted_iota(jnp.int32, (half, half), 0) >= lax.broadcasted_iota(jnp.int32, (half, half), 1)
    lo = qkv_ref[side, 0]
    hi = qkv_ref[1 - side, 0]
    lo_outs, hi_outs = [], []
    for head in range(qkv_ref.shape[3] // (3 * head_dim)):
        base = head * 3 * head_dim
        q_lo, k_lo, v_lo = (lo[:, base + part * head_dim:base + (part + 1) * head_dim] for part in range(3))
        q_hi, k_hi, v_hi = (hi[:, base + part * head_dim:base + (part + 1) * head_dim] for part in range(3))

        scores = jnp.where(diag, dot_nt(q_lo, k_lo), -1e30)
        top = jnp.max(scores, axis=1, keepdims=True)
        expo = jnp.exp2((scores - top) * exponent)
        prob = (expo * (1.0 / jnp.sum(expo, axis=1, keepdims=True))).astype(BF16)
        lo_outs.append(dot_nn(prob, v_lo).astype(BF16))

        past = dot_nt(q_hi, k_lo)
        scores = jnp.where(diag, dot_nt(q_hi, k_hi), -1e30)
        top = jnp.maximum(jnp.max(past, axis=1, keepdims=True), jnp.max(scores, axis=1, keepdims=True))
        past = jnp.exp2((past - top) * exponent)
        expo = jnp.exp2((scores - top) * exponent)
        scale = 1.0 / (jnp.sum(past, axis=1, keepdims=True) + jnp.sum(expo, axis=1, keepdims=True))
        out = dot_nn((past * scale).astype(BF16), v_lo) + dot_nn((expo * scale).astype(BF16), v_hi)
        hi_outs.append(out.astype(BF16))
    out_ref[side, 0] = jnp.concatenate(lo_outs, axis=1)
    out_ref[1 - side, 0] = jnp.concatenate(hi_outs, axis=1)


def attend_back_kernel(head_dim, side_ref, qkv_ref, d_att_ref, d_qkv_ref, sum_ref):
    side = side_ref[0]
    half = qkv_ref.shape[2]
    inv_root = head_dim ** -0.5
    exponent = inv_root * math.log2(math.e)
    diag = lax.broadcasted_iota(jnp.int32, (half, half), 1) >= lax.broadcasted_iota(jnp.int32, (half, half), 0)
    lo = qkv_ref[side, 0]
    hi = qkv_ref[1 - side, 0]
    d_lo = d_att_ref[side, 0]
    d_hi = d_att_ref[1 - side, 0]
    lo_outs, hi_outs = [], []
    for head in range(qkv_ref.shape[3] // (3 * head_dim)):
        base = head * 3 * head_dim
        q_lo, k_lo, v_lo = (lo[:, base + part * head_dim:base + (part + 1) * head_dim] for part in range(3))
        q_hi, k_hi, v_hi = (hi[:, base + part * head_dim:base + (part + 1) * head_dim] for part in range(3))
        do_lo = d_lo[:, head * head_dim:(head + 1) * head_dim]
        do_hi = d_hi[:, head * head_dim:(head + 1) * head_dim]

        scores = jnp.where(diag, dot_nt(k_lo, q_lo), -1e30)
        expo = jnp.exp2((scores - jnp.max(scores, axis=0, keepdims=True)) * exponent)
        prob = expo * (1.0 / jnp.sum(expo, axis=0, keepdims=True))
        d_prob = dot_nt(v_lo, do_lo)
        mean = jnp.sum(d_prob * prob, axis=0, keepdims=True)
        d_scores = (prob * (d_prob - mean)).astype(BF16)
        dv_lo = dot_nn(prob.astype(BF16), do_lo)
        dk_lo = dot_nn(d_scores, q_lo)
        dq_lo = dot_tn(d_scores, k_lo) * inv_root

        past = dot_nt(k_lo, q_hi)
        scores = jnp.where(diag, dot_nt(k_hi, q_hi), -1e30)
        top = jnp.maximum(jnp.max(past, axis=0, keepdims=True), jnp.max(scores, axis=0, keepdims=True))
        past = jnp.exp2((past - top) * exponent)
        expo = jnp.exp2((scores - top) * exponent)
        scale = 1.0 / (jnp.sum(past, axis=0, keepdims=True) + jnp.sum(expo, axis=0, keepdims=True))
        past = past * scale
        expo = expo * scale
        d_past = dot_nt(v_lo, do_hi)
        d_prob = dot_nt(v_hi, do_hi)
        mean = jnp.sum(d_past * past, axis=0, keepdims=True) + jnp.sum(d_prob * expo, axis=0, keepdims=True)
        d_past = (past * (d_past - mean)).astype(BF16)
        d_scores = (expo * (d_prob - mean)).astype(BF16)
        dv_lo = dv_lo + dot_nn(past.astype(BF16), do_hi)
        dv_hi = dot_nn(expo.astype(BF16), do_hi)
        dk_lo = (dk_lo + dot_nn(d_past, q_hi)) * inv_root
        dk_hi = dot_nn(d_scores, q_hi) * inv_root
        dq_hi = (dot_tn(d_past, k_lo) + dot_tn(d_scores, k_hi)) * inv_root
        lo_outs += [dq_lo, dk_lo, dv_lo]
        hi_outs += [dq_hi, dk_hi, dv_hi]
    lo_all = jnp.concatenate(lo_outs, axis=1)
    hi_all = jnp.concatenate(hi_outs, axis=1)
    d_qkv_ref[side, 0] = lo_all.astype(BF16)
    d_qkv_ref[1 - side, 0] = hi_all.astype(BF16)
    both = lo_all + hi_all
    sum_ref[0] = jnp.sum(both.reshape(half // 8, 8, both.shape[1]), axis=0)


def attend(side, qkv, head_dim):
    _, batch, half, width = qkv.shape
    pairs = width // (6 * head_dim)
    flops = 2 * 4 * batch * half * half * width
    return pl.pallas_call(
        functools.partial(attend_kernel, head_dim),
        grid_spec=pltpu.PrefetchScalarGridSpec(
            num_scalar_prefetch=1,
            grid=(batch, pairs),
            in_specs=[pl.BlockSpec((2, 1, half, 6 * head_dim), lambda b, h, s: (0, b, 0, h))],
            out_specs=pl.BlockSpec((2, 1, half, 2 * head_dim), lambda b, h, s: (0, b, 0, h)),
        ),
        out_shape=jax.ShapeDtypeStruct((2, batch, half, width // 3), BF16),
        cost_estimate=pl.CostEstimate(flops=flops * 4, bytes_accessed=qkv.size * 3, transcendentals=0),
        compiler_params=pltpu.CompilerParams(dimension_semantics=('parallel', 'parallel')),
    )(side, qkv)


def attend_back(side, qkv, d_att, head_dim):
    _, batch, half, width = qkv.shape
    pairs = width // (6 * head_dim)
    flops = 2 * 4 * batch * half * half * width
    return pl.pallas_call(
        functools.partial(attend_back_kernel, head_dim),
        grid_spec=pltpu.PrefetchScalarGridSpec(
            num_scalar_prefetch=1,
            grid=(batch, pairs),
            in_specs=[
                pl.BlockSpec((2, 1, half, 6 * head_dim), lambda b, h, s: (0, b, 0, h)),
                pl.BlockSpec((2, 1, half, 2 * head_dim), lambda b, h, s: (0, b, 0, h)),
            ],
            out_specs=[
                pl.BlockSpec((2, 1, half, 6 * head_dim), lambda b, h, s: (0, b, 0, h)),
                pl.BlockSpec((1, 8, 6 * head_dim), lambda b, h, s: (b, 0, h)),
            ],
        ),
        out_shape=[
            jax.ShapeDtypeStruct(qkv.shape, BF16),
            jax.ShapeDtypeStruct((batch, 8, width), F32),
        ],
        cost_estimate=pl.CostEstimate(flops=flops * 10, bytes_accessed=qkv.size * 5, transcendentals=0),
        compiler_params=pltpu.CompilerParams(dimension_semantics=('parallel', 'parallel')),
    )(side, qkv, d_att)


def gather_fsdp(part):
    return lax.all_gather(part, FSDP, axis=0, tiled=True)


def gather_all(part):
    return lax.all_gather(part, ALL, axis=0, tiled=True)


def swap(values):
    return lax.ppermute(values, 'tp', SWAP)


def scatter_rows(part_sum, row_dim):
    return lax.psum_scatter(part_sum, FSDP, scatter_dimension=row_dim, tiled=True)


def scatter_pair(tp_index, rows, tp_dim):
    size = rows.shape[tp_dim] // 2
    keep = lax.dynamic_slice_in_dim(rows, tp_index * size, size, tp_dim)
    give = lax.dynamic_slice_in_dim(rows, (1 - tp_index) * size, size, tp_dim)
    return keep + swap(give)


def local_layer(x_loc, dy_loc, ln1_gain, ln1_bias, w_qkv, b_qkv, w_out, b_out, ln2_gain, ln2_bias, w_up, b_up, w_down, b_down):
    tp_index = lax.axis_index('tp')
    side = jnp.reshape(tp_index, (1,)).astype(jnp.int32)
    batch = x_loc.shape[0] // 2
    half, width = x_loc.shape[1], x_loc.shape[2]
    heads, qkv_width = w_qkv.shape[1], w_qkv.shape[2]
    head_dim = qkv_width // 3

    def exchange(values):
        own = lax.dynamic_slice_in_dim(values, tp_index * batch, batch, 0)
        other = swap(lax.dynamic_slice_in_dim(values, (1 - tp_index) * batch, batch, 0))
        return jnp.stack([own, other])

    def restore(own, other):
        out = jnp.zeros((2 * batch, half, width), own.dtype)
        out = lax.dynamic_update_slice_in_dim(out, own, tp_index * batch, 0)
        return lax.dynamic_update_slice_in_dim(out, other, (1 - tp_index) * batch, 0)

    def gather_columns(part):
        columns = part.shape[1]
        both = jnp.zeros((part.shape[0], 2 * columns), part.dtype)
        both = lax.dynamic_update_slice_in_dim(both, part, tp_index * columns, 1)
        both = lax.dynamic_update_slice_in_dim(both, swap(part), (1 - tp_index) * columns, 1)
        return gather_fsdp(both)

    def rows(values):
        return values.reshape(2 * batch * half, values.shape[-1])

    def cube(values):
        return values.reshape(2, batch, half, values.shape[-1])

    def pair(values):
        return values.reshape(2, values.shape[0] // 2, values.shape[1])

    qkv_weight = gather_columns(w_qkv.reshape(w_qkv.shape[0], heads * qkv_width))
    x_all = exchange(x_loc)
    vectors = (ln1_gain, ln1_bias, b_out, ln2_gain, ln2_bias, b_down, b_qkv, b_up)
    sizes = [vector.shape[0] for vector in vectors]
    gathered = [gather_all(vector).astype(F32) for vector in vectors]
    gain_one, bias_one, bias_out, gain_two, bias_two, bias_down = (whole[:whole.shape[0] // 2] for whole in gathered[:6])
    qkv_bias, up_bias = gathered[6:]
    out_weight = gather_all(w_out)
    up_weight = gather_columns(w_up)
    down_weight = gather_all(w_down)
    dy_low = rows(exchange(dy_loc))

    x_wide = rows(x_all).astype(F32)
    ln1_val, ln1_back = jax.vjp(layer_norm, x_wide, gain_one, bias_one)
    h_one = ln1_val.astype(BF16)
    qkv = cube((dot_nn(h_one, qkv_weight) + qkv_bias).astype(BF16))
    att = rows(attend(side, qkv, head_dim))
    residual = x_wide + dot_nn(att, out_weight) + bias_out
    ln2_val, ln2_back = jax.vjp(layer_norm, residual, gain_two, bias_two)
    h_two = ln2_val.astype(BF16)
    gelu_out, gelu_back = jax.vjp(gelu_tanh, dot_nn(h_two, up_weight) + up_bias)
    gelu_low = gelu_out.astype(BF16)
    y_all = (residual + dot_nn(gelu_low, down_weight) + bias_down).astype(BF16)
    y_all, dy_low = lax.optimization_barrier((y_all, dy_low))
    y_other = swap(cube(y_all)[1])

    dy_wide = dy_low.astype(F32)
    part_down = dot_tn(gelu_low, dy_low)
    d_up = gelu_back(dot_nt(dy_low, down_weight))[0]
    d_up_low = d_up.astype(BF16)
    g_b_up = jnp.sum(d_up, axis=0)
    d_up_low, part_down = lax.optimization_barrier((d_up_low, part_down))
    part_up = dot_tn(h_two, d_up_low)
    d_up_low, part_up = lax.optimization_barrier((d_up_low, part_up))
    d_res_ln, g_gain_two, g_bias_two = ln2_back(dot_nt(d_up_low, up_weight))
    d_resid = dy_wide + d_res_ln
    g_b_out = jnp.sum(d_resid, axis=0)
    d_resid_low = d_resid.astype(BF16)
    part_out = dot_tn(att, d_resid_low)
    d_resid_low, part_out = lax.optimization_barrier((d_resid_low, part_out))
    d_att = cube(dot_nt(d_resid_low, out_weight).astype(BF16))
    grad_w_down = scatter_pair(tp_index, scatter_rows(pair(part_down), 1), 0)[0]
    rows_up = scatter_rows(part_up, 0)
    d_att, grad_w_down = lax.optimization_barrier((d_att, grad_w_down))
    d_qkv_low, d_qkv_sum = attend_back(side, qkv, d_att, head_dim)
    d_qkv_low = rows(d_qkv_low)
    d_qkv_low, rows_up, y_other = lax.optimization_barrier((d_qkv_low, rows_up, y_other))
    y_loc = restore(cube(y_all)[0], y_other)
    grad_w_up = scatter_pair(tp_index, rows_up, 1)
    part_qkv = dot_tn(h_one, d_qkv_low)
    d_qkv_low, part_qkv = lax.optimization_barrier((d_qkv_low, part_qkv))
    d_x_ln, g_gain_one, g_bias_one = ln1_back(dot_nt(d_qkv_low, qkv_weight))
    dx_all = cube((d_resid + d_x_ln).astype(BF16))
    dx_loc = restore(dx_all[0], swap(dx_all[1]))

    grad_w_out = scatter_pair(tp_index, scatter_rows(pair(part_out), 1), 0)[0]
    grad_w_qkv = scatter_pair(tp_index, scatter_rows(part_qkv, 0), 1).reshape(w_qkv.shape)
    fsdp_index = lax.axis_index(FSDP)
    sums = (g_gain_one, g_bias_one, g_b_out, g_gain_two, g_bias_two, jnp.sum(dy_wide, axis=0), jnp.sum(d_qkv_sum, axis=(0, 1)), g_b_up)
    totals = lax.psum(sums, ALL)
    shares = []
    for place, size in enumerate(sizes):
        rank = fsdp_index if place < 6 else tp_index * (sums[place].shape[0] // (2 * size)) + fsdp_index
        shares.append(lax.dynamic_slice_in_dim(totals[place], rank * size, size, 0))
    grad_ln1_gain, grad_ln1_bias, grad_b_out, grad_ln2_gain, grad_ln2_bias, grad_b_down, grad_b_qkv, grad_b_up = shares
    return (y_loc, dx_loc, grad_ln1_gain, grad_ln1_bias, grad_w_qkv, grad_b_qkv, grad_w_out, grad_b_out, grad_ln2_gain, grad_ln2_bias, grad_w_up, grad_b_up, grad_w_down, grad_b_down)


def solution(mesh):
    fine = Mesh(mesh.devices.reshape(2, 2, 2, 2), ALL)
    act_spec = P(FSDP, 'tp', None)
    vec_spec = P(FSDP)
    split_spec = P(ALL)
    row_spec = P(ALL, None)
    param_specs = (vec_spec, vec_spec, P(FSDP, 'tp', None), split_spec, row_spec, vec_spec, vec_spec, vec_spec, P(FSDP, 'tp'), split_spec, row_spec, vec_spec)
    return jax.shard_map(local_layer, mesh=fine, in_specs=(act_spec, act_spec) + param_specs, out_specs=(act_spec, act_spec) + param_specs, check_vma=False)
```
